16 devices in a mesh: dp: 4 (over y, z, core), tp: 4 (over x).
Axes of the slice: x: 4, y: 2, z: 1, core: 2. Of those that a mesh axis runs over, the one named last changes fastest.
The devices are a block of a 4x4x4 slice.
Arguments:
- x: bfloat16 [256, 5120], P('dp'), parts along dimension 0
- k_cache: bfloat16 [256, 2048, 8, 160], P('dp', None, 'tp'), parts along dimension 0
- v_cache: bfloat16 [256, 2048, 8, 160], P('dp', None, 'tp'), parts along dimension 0
- gain_a: bfloat16 [5120], replicated
- wq: bfloat16 [5120, 5120], P(None, 'tp')
- wo: bfloat16 [5120, 5120], P('tp')
- gain_m: bfloat16 [5120], replicated
- w_gate: bfloat16 [5120, 13824], P(None, 'tp')
- w_up: bfloat16 [5120, 13824], P(None, 'tp')
- w_down: bfloat16 [13824, 5120], P('tp')
Outputs:
- output: bfloat16 [256, 5120], P('dp'), parts along dimension 0
There are 4 independent parts. The reference program is written for one: setup_inputs(seed, part) draws one part's arguments, and reference() takes and returns one part's arrays. A program takes and returns all parts, laid end to end along the dimension named above; an argument that names none is the same for every part.
All inputs are finite; a program needn't handle non-finite values.
Results may differ from the reference program's by a relative error of at most 0.017.
Values are sent between devices in bfloat16 or wider.
A program may use at most 1.5 GiB of HBM per device.

```python
import jax
import jax.numpy as jnp
from jax import lax

BATCH = 64
CACHE = 2048
D = 5120
HEADS = 32
KV_HEADS = 8
HEAD = 160
FF = 13824
THETA = 10000


def setup_inputs(seed: int = 0, part: int = 0) -> dict:
    kx, kc, kw, kn, kq, ko, km, kg, ku, kd = jax.random.split(jax.random.key(seed), 10)
    kx, kc, kw = (jax.random.fold_in(k, part) for k in (kx, kc, kw))

    def weights(key, rows, columns):
        return jax.random.normal(key, (rows, columns), jnp.float32) * rows**-0.5

    drawn = {
        "x": jax.random.normal(kx, (BATCH, D), jnp.float32),
        "k_cache": 2 * jax.random.normal(kc, (BATCH, CACHE, KV_HEADS, HEAD), jnp.float32),
        "v_cache": 4 * jax.random.normal(kw, (BATCH, CACHE, KV_HEADS, HEAD), jnp.float32),
        "gain_a": 1 + 0.1 * jax.random.normal(kn, (D,), jnp.float32),
        "wq": 2 * weights(kq, D, HEADS * HEAD),
        "wo": weights(ko, HEADS * HEAD, D),
        "gain_m": 1 + 0.1 * jax.random.normal(km, (D,), jnp.float32),
        "w_gate": weights(kg, D, FF),
        "w_up": weights(ku, D, FF),
        "w_down": 2 * weights(kd, FF, D),
    }
    return {k: v.astype(jnp.bfloat16) for k, v in drawn.items()}


def normed(x, gain):
    wide = x.astype(jnp.float32)
    scale = lax.rsqrt(jnp.mean(wide * wide, -1, keepdims=True) + 1e-6)
    return (wide * scale * gain.astype(jnp.float32)).astype(jnp.bfloat16)


def turned(t, place, theta):
    half = t.shape[-1] // 2
    angle = place.astype(jnp.float32)[:, None] * theta ** (-jnp.arange(half, dtype=jnp.float32) / half)
    cos, sin = jnp.cos(angle)[:, None], jnp.sin(angle)[:, None]
    a, b = t[..., :half].astype(jnp.float32), t[..., half:].astype(jnp.float32)
    return jnp.concatenate([a * cos - b * sin, b * cos + a * sin], -1).astype(jnp.bfloat16)


def matmul(a, w):
    return jnp.dot(a, w, preferred_element_type=jnp.float32).astype(jnp.bfloat16)


def einsum(form, a, b):
    return jnp.einsum(form, a.astype(jnp.float32), b.astype(jnp.float32))


def seen_by(a, wq, k_cache, v_cache, head, theta):
    batch, cache, kv_heads = k_cache.shape[:3]
    place = jnp.full((batch,), cache - 1)
    q = turned(matmul(a, wq).reshape(batch, -1, head), place, theta).reshape(batch, kv_heads, -1, head)
    scores = einsum("bgsd,bugd->bgsu", q, k_cache) * head**-0.5
    weights = jax.nn.softmax(scores, -1).astype(jnp.bfloat16)
    return einsum("bgsu,bugd->bgsd", weights, v_cache).astype(jnp.bfloat16).reshape(batch, -1)


def hidden_of(b, w_gate, w_up):
    gate = jnp.dot(b, w_gate, preferred_element_type=jnp.float32)
    up = jnp.dot(b, w_up, preferred_element_type=jnp.float32)
    return (jax.nn.silu(gate) * up).astype(jnp.bfloat16)


def reference(x, k_cache, v_cache, gain_a, wq, wo, gain_m, w_gate, w_up, w_down):
    seen = seen_by(normed(x, gain_a), wq, k_cache, v_cache, HEAD, THETA)
    h = (x.astype(jnp.float32) + jnp.dot(seen, wo, preferred_element_type=jnp.float32)).astype(jnp.bfloat16)
    hidden = hidden_of(normed(h, gain_m), w_gate, w_up)
    return (h.astype(jnp.float32) + jnp.dot(hidden, w_down, preferred_element_type=jnp.float32)).astype(jnp.bfloat16)
```

```python
import functools

import jax
import jax.numpy as jnp
import numpy as np
from jax import lax
from jax.experimental import pallas as pl
from jax.experimental.pallas import tpu as pltpu
from jax.sharding import PartitionSpec as P

HEAD = 160
THETA = 10000
F32, BF16 = jnp.float32, jnp.bfloat16
MESH = pl.DeviceIdType.MESH

BATCH = 4
RING = 3
UNIT = 1280
UNITS = 10
WIDE = 2048
SLAB = 320
CHUNK = 512
LOW = 1664
GROUPS = ((0, 12), (12, 16))
WO_AT = 6
SPLIT_UNIT = 8


def many(v, n):
    return pl.multiple_of(v, n)


def kernel(dims, x_hbm, k_hbm, v_hbm, ga_hbm, wq_hbm, wo_hbm, gm_hbm, wg_hbm, wu_hbm, wd_hbm, turn_hbm, out_hbm, *scratch):
    rows, d, cache, heads, kv_heads, ff = dims
    (pool, x_s, ga_s, gm_s, turn_s, ab, qs, os, seen, part, accu, st1, rv1, st2, rv2, h_s, y_s, hid, rv1b, st2b, rv2b,
     misc_sem, wq_sem, kv_sem, wo_sem, slab_sem, wd_sem, out_sem, a1_send, a1_recv, a2_send, a2_recv) = scratch
    kvd = kv_heads * HEAD
    tiles = -(-kvd // 128)
    qd = heads * HEAD
    share = heads // kv_heads
    batches = rows // BATCH
    slabs = d // SLAB
    chunks = d // CHUNK
    last = slabs - UNITS

    me = lax.axis_index("tp")
    beside = me + 1 - 2 * lax.rem(me, 2)
    across = 3 - me
    barrier = pltpu.get_barrier_semaphore()
    for other in (beside, across):
        pl.semaphore_signal(barrier, inc=1, device_id={"tp": other}, device_id_type=MESH)
    plan = (
        (beside, across, lax.rem((me + 1) // 2, 2), me // 2),
        (across, beside, me // 2, lax.rem(me, 2)),
    )

    x_copy = pltpu.make_async_copy(x_hbm, x_s, misc_sem.at[0])
    ga_copy = pltpu.make_async_copy(ga_hbm, ga_s, misc_sem.at[1])
    gm_copy = pltpu.make_async_copy(gm_hbm, gm_s, misc_sem.at[2])
    turn_copy = pltpu.make_async_copy(turn_hbm, turn_s, misc_sem.at[3])

    def wq_copy(i):
        return pltpu.make_async_copy(
            wq_hbm.at[pl.ds(i * UNIT, UNIT)], pool.at[pl.ds((WO_AT + i) * UNIT, UNIT), pl.ds(0, qd)], wq_sem.at[i]
        )

    def kv_at(i):
        return many(lax.rem(i + 2, RING) * (2 * UNIT), UNIT)

    def kv_copies(i):
        slot = lax.rem(i + 2, RING)
        n = BATCH * kvd
        return [
            pltpu.make_async_copy(src.at[pl.ds(many(i * n, n), n)], pool.at[pl.ds(kv_at(i) + j * UNIT, n)], kv_sem.at[slot, j])
            for j, src in enumerate((k_hbm, v_hbm))
        ]

    def wo_copies():
        return [
            pltpu.make_async_copy(
                wo_hbm.at[:, pl.ds(j * WIDE, w)], pool.at[pl.ds((WO_AT + j) * UNIT, qd), pl.ds(0, w)], wo_sem.at[j]
            )
            for j, w in enumerate((WIDE, WIDE, d - 2 * WIDE))
        ]

    def slab_copies(k):
        unit = lax.rem(k + UNITS - 1, UNITS)
        copies = []
        for m, src in enumerate((wg_hbm, wu_hbm)):
            for j, w in enumerate((WIDE, ff - WIDE)):
                p = 2 * m + j
                copies.append(
                    pltpu.make_async_copy(
                        src.at[pl.ds(many(k * SLAB, SLAB), SLAB), pl.ds(j * WIDE, w)],
                        pool.at[pl.ds(many(unit * UNIT, UNIT) + p * SLAB, SLAB), pl.ds(0, w)],
                        slab_sem.at[unit, p],
                    )
                )
        return copies

    def start(copies):
        for c in copies:
            c.start()

    def wait(copies, name):
        with jax.named_scope(name):
            for c in copies:
                c.wait()

    def chunk_place(pos):
        over4, over6 = (pos + 4) // 8, (pos + 2) // 8
        split = over4 - over6
        chunk = pos + 4 * split - 2 * over6
        row = UNIT * (5 * (1 - over4) + SPLIT_UNIT * split)
        lane = (pos - 4 * split - 6 * over6) * CHUNK
        return chunk, (row, lane), (row + LOW * (1 - split), lane + 2 * CHUNK * split)

    def chunk_copies(pos):
        chunk, low, high = chunk_place(pos)
        cols = pl.ds(many(chunk * CHUNK, CHUNK), CHUNK)
        return [
            pltpu.make_async_copy(
                wd_hbm.at[pl.ds(at, n), cols],
                pool.at[pl.ds(many(row, 128), n), pl.ds(many(lane, CHUNK), CHUNK)],
                wd_sem.at[pos, j],
            )
            for j, (at, n, (row, lane)) in enumerate(((0, LOW, low), (LOW, ff - LOW, high)))
        ]

    x_copy.start()
    ga_copy.start()
    turn_copy.start()
    for i in range(d // UNIT):
        wq_copy(i).start()
    for i in range(RING):
        start(kv_copies(i))
    gm_copy.start()

    @jax.named_scope("norm")
    def norm(src, gain_ref, row0, n):
        g = gain_ref[...].astype(F32)
        gain = jnp.concatenate([g[r : r + 1] for r in range(g.shape[0])], axis=1)

        def body(i, _):
            at = pl.ds(many(row0 + i * 16, 16), 16)
            wide = src[at, :].astype(F32)
            scale = lax.rsqrt(jnp.mean(wide * wide, -1, keepdims=True) + 1e-6)
            out = (wide * scale * gain).astype(BF16)
            for k in range(slabs):
                ab[k, at, :] = out[:, k * SLAB : (k + 1) * SLAB]
            return 0

        lax.fori_loop(0, n // 16, body, 0)

    x_copy.wait()
    ga_copy.wait()
    norm(x_s, ga_s, 0, rows)

    per = UNIT // SLAB
    for i in range(d // UNIT):
        wq_copy(i).wait()
        total = None
        for j in range(per):
            term = jnp.dot(
                ab[i * per + j], pool[(WO_AT + i) * UNIT + j * SLAB : (WO_AT + i) * UNIT + (j + 1) * SLAB, :qd],
                preferred_element_type=F32,
            )
            total = term if total is None else total + term
        part[:, :qd] = total if i == 0 else part[:, :qd] + total
    turn_copy.wait()
    cos, sin = turn_s[0:1, :], turn_s[1:2, :]
    blank = jnp.zeros((rows, HEAD), F32)
    for j in range(heads):
        t = part[:, j * HEAD : (j + 1) * HEAD].astype(BF16).astype(F32)
        swapped = jnp.concatenate([t[:, HEAD // 2 :], t[:, : HEAD // 2]], axis=1)
        t = (t * cos + swapped * sin).astype(BF16).astype(F32)
        side = [blank] * kv_heads
        side[j // share] = t
        t = jnp.concatenate(side + [jnp.zeros((rows, tiles * 128 - kvd), F32)], axis=1)
        for c in range(tiles):
            qs[c, pl.ds(j, rows, stride=heads), :] = t[:, c * 128 : (c + 1) * 128]

    half1, piece1, quarter1 = d // 2, d // 4, d // 8

    def first_copy(g, step, half):
        b0, b1 = GROUPS[g]
        at = pl.ds(b0 * BATCH, (b1 - b0) * BATCH)
        p1, p2, bit1, bit2 = plan[half]
        base = half * half1
        keep = base + bit1 * piece1
        if step == 0:
            src = st1.at[at, pl.ds(many(base + (1 - bit1) * piece1, 128), piece1)]
            dst, to = rv1.at[at, pl.ds(half * piece1, piece1)], p1
        elif step == 1:
            src = st2.at[at, pl.ds(half * quarter1, quarter1)]
            dst, to = rv2.at[at, pl.ds(half * quarter1, quarter1)], p2
        elif step == 2:
            src = dst = h_s.at[at, pl.ds(many(keep + bit2 * quarter1, 128), quarter1)]
            to = p2
        else:
            src = dst = h_s.at[at, pl.ds(many(keep, 128), piece1)]
            to = p1
        return pltpu.make_async_remote_copy(
            src_ref=src, dst_ref=dst, send_sem=a1_send.at[g, step, half], recv_sem=a1_recv.at[g, step, half],
            device_id={"tp": to}, device_id_type=MESH,
        )

    @jax.named_scope("first_step")
    def first_step(g, step):
        b0, b1 = GROUPS[g]
        at = slice(b0 * BATCH, b1 * BATCH)
        for half in range(2):
            p1, p2, bit1, bit2 = plan[half]
            base = half * half1
            keep = base + bit1 * piece1
            if step == 0:
                away = pl.ds(many(base + (1 - bit1) * piece1, 128), piece1)
                st1[at, away] = part[at, away].astype(BF16)
                first_copy(g, 0, half).start()
                continue
            first_copy(g, step - 1, half).wait_recv()
            if step == 1:
                off = (1 - bit2) * quarter1
                st2[at, half * quarter1 : (half + 1) * quarter1] = (
                    part[at, pl.ds(many(keep + off, 128), quarter1)]
                    + rv1[at, pl.ds(many(half * piece1 + off, 128), quarter1)].astype(F32)
                ).astype(BF16)
                first_copy(g, 1, half).start()
            elif step == 2:
                mine = pl.ds(many(keep + bit2 * quarter1, 128), quarter1)
                h_s[at, mine] = (
                    x_s[at, mine].astype(F32)
                    + part[at, mine]
                    + rv1[at, pl.ds(many(half * piece1 + bit2 * quarter1, 128), quarter1)].astype(F32)
                    + rv2[at, half * quarter1 : (half + 1) * quarter1].astype(F32)
                ).astype(BF16)
                first_copy(g, 2, half).start()
            elif step == 3:
                first_copy(g, 3, half).start()

    def first_sends(g):
        for half in range(2):
            for step in range(4):
                first_copy(g, step, half).wait_send()

    @jax.named_scope("project")
    def project(g):
        b0, b1 = GROUPS[g]
        n = (b1 - b0) * BATCH
        at = slice(b0 * BATCH, b1 * BATCH)
        for j in range(heads):
            o = jnp.concatenate([os[c, pl.ds(b0 * BATCH * heads + j, n, stride=heads), :] for c in range(tiles)], axis=1)
            h = j // share
            seen[at, j * HEAD : (j + 1) * HEAD] = o[:, h * HEAD : (h + 1) * HEAD].astype(BF16)
        lhs = seen[at, :]

        def body(c, _):
            row, lane = (WO_AT + c // 2) * UNIT, lax.rem(c, 2) * (WIDE // 2)
            w = pool[pl.ds(many(row, UNIT), qd), pl.ds(many(lane, WIDE // 2), WIDE // 2)]
            part[at, pl.ds(many(c * (WIDE // 2), WIDE // 2), WIDE // 2)] = jnp.dot(lhs, w, preferred_element_type=F32)
            return 0

        lax.fori_loop(0, d // (WIDE // 2), body, 0)

    def attend(i, _):
        wait(kv_copies(i), "kv_wait")
        at = kv_at(i)
        ws = []
        for j in range(BATCH):
            mine = pl.ds(many((i * BATCH + j) * heads, 8), heads)
            q = jnp.concatenate([qs[c, mine, :] for c in range(tiles)], axis=1)[:, :kvd].astype(BF16)
            scores = jnp.dot(q, pool[pl.ds(at + j * kvd, kvd), :], preferred_element_type=F32) * HEAD**-0.5
            top = jnp.max(scores, -1, keepdims=True)
            e = jnp.exp(scores - top)
            ws.append(e / jnp.sum(e, -1, keepdims=True))
        w = jnp.concatenate(ws, 0).astype(BF16)
        o = lax.dot_general(w, pool[pl.ds(at + UNIT, BATCH * kvd), :], (((1,), (1,)), ((), ())), preferred_element_type=F32)
        for j in range(BATCH):
            t = o[j * heads : (j + 1) * heads, j * kvd : (j + 1) * kvd]
            t = jnp.concatenate([t, jnp.zeros((heads, tiles * 128 - kvd), F32)], axis=1)
            for c in range(tiles):
                os[c, pl.ds(many((i * BATCH + j) * heads, 8), heads), :] = t[:, c * 128 : (c + 1) * 128]

        @pl.when(i + RING < batches)
        def _():
            start(kv_copies(i + RING))

        @pl.when(i == 5)
        def _():
            start(wo_copies())

        end0 = GROUPS[0][1]

        @pl.when(i == end0 - 1)
        def _():
            wait(wo_copies(), "wo_wait")
            project(0)
            pl.semaphore_wait(barrier, 2)
            first_step(0, 0)

        for step in range(1, 4):

            @pl.when(i == end0 - 1 + step)
            def _():
                first_step(0, step)

        @pl.when(i == batches - RING - 1)
        def _():
            start(slab_copies(0))

        @pl.when(i >= batches - RING)
        def _():
            k = 1 + 2 * (i - (batches - RING))
            start(slab_copies(k))
            start(slab_copies(k + 1))

        return 0

    lax.fori_loop(0, batches, attend, 0)

    project(1)
    first_step(1, 0)
    for k in range(2 * RING + 1, UNITS):
        start(slab_copies(k))
    for half in range(2):
        first_copy(0, 3, half).wait_recv()
    gm_copy.wait()
    b0, b1 = GROUPS[0]
    norm(h_s, gm_s, b0 * BATCH, (b1 - b0) * BATCH)
    for step in range(1, 4):
        first_step(1, step)
    accu[...] = jnp.zeros_like(accu)
    for half in range(2):
        first_copy(1, 3, half).wait_recv()
    first_sends(0)
    first_sends(1)
    part[:, :ff] = jnp.zeros((rows, ff), F32)
    b0, b1 = GROUPS[1]
    norm(h_s, gm_s, b0 * BATCH, (b1 - b0) * BATCH)

    def slab_body(k, _):
        unit = lax.rem(k + UNITS - 1, UNITS)
        wait(slab_copies(k), "slab_wait")
        lhs = ab[k]
        for m, acc in enumerate((part, accu)):
            for j, w in enumerate((WIDE, ff - WIDE)):
                at = pl.ds(many(unit * UNIT, UNIT) + (2 * m + j) * SLAB, SLAB)
                acc[:, j * WIDE : j * WIDE + w] += jnp.dot(lhs, pool[at, :w], preferred_element_type=F32)

        @pl.when(k < last)
        def _():
            start(slab_copies(k + UNITS))

        for after, first, n in ((8, 0, 4), (10, 4, 2), (13, 6, 4)):

            @pl.when(k == after)
            def _():
                for pos in range(first, first + n):
                    start(chunk_copies(pos))

        return 0

    lax.fori_loop(0, slabs, slab_body, 0)

    @jax.named_scope("hidden")
    def hidden_body(c, _):
        at = pl.ds(many(c * 384, 128), 384)
        hid[:, at] = (jax.nn.silu(part[:, at]) * accu[:, at]).astype(BF16)
        return 0

    lax.fori_loop(0, ff // 384, hidden_body, 0)

    side = CHUNK // 2

    def second_copy(pos, step, half):
        chunk, _, _ = chunk_place(pos)
        p1, p2, bit1, bit2 = plan[half]
        cols = pl.ds(many(chunk * CHUNK + half * side, side), side)
        if step == 0:
            src = st1.at[pl.ds(many((1 - bit1) * (rows // 2), 16), rows // 2), cols]
            dst, to = rv1b.at[pos, half], p1
        elif step == 1:
            src, dst, to = st2b.at[pos, half], rv2b.at[pos, half], p2
        elif step == 2:
            src = dst = y_s.at[pl.ds(many(bit1 * (rows // 2) + bit2 * (rows // 4), 16), rows // 4), cols]
            to = p2
        else:
            src = dst = y_s.at[pl.ds(many(bit1 * (rows // 2), 16), rows // 2), cols]
            to = p1
        return pltpu.make_async_remote_copy(
            src_ref=src, dst_ref=dst, send_sem=a2_send.at[pos, step, half], recv_sem=a2_recv.at[pos, step, half],
            device_id={"tp": to}, device_id_type=MESH,
        )

    @jax.named_scope("second_step")
    def second_step(pos, step):
        chunk, _, _ = chunk_place(pos)
        for half in range(2):
            p1, p2, bit1, bit2 = plan[half]
            cols = pl.ds(many(chunk * CHUNK + half * side, side), side)
            second_copy(pos, step - 1, half).wait_recv()
            if step == 1:
                off = (1 - bit2) * (rows // 4)
                st2b[pos, half] = (
                    part[pl.ds(many(bit1 * (rows // 2) + off, 16), rows // 4), cols]
                    + rv1b[pos, half, pl.ds(many(off, 16), rows // 4), :].astype(F32)
                ).astype(BF16)
                second_copy(pos, 1, half).start()
            elif step == 2:
                mine = pl.ds(many(bit1 * (rows // 2) + bit2 * (rows // 4), 16), rows // 4)
                y_s[mine, cols] = (
                    h_s[mine, cols].astype(F32)
                    + part[mine, cols]
                    + rv1b[pos, half, pl.ds(many(bit2 * (rows // 4), 16), rows // 4), :].astype(F32)
                    + rv2b[pos, half].astype(F32)
                ).astype(BF16)
                second_copy(pos, 2, half).start()
            elif step == 3:
                second_copy(pos, 3, half).start()

    def out_copy(pos):
        chunk, _, _ = chunk_place(pos)
        cols = pl.ds(many(chunk * CHUNK, CHUNK), CHUNK)
        return pltpu.make_async_copy(y_s.at[:, cols], out_hbm.at[:, cols], out_sem.at[pos])

    lag = 2

    def down_body(pos, _):
        @pl.when(pos >= 4 * lag)
        def _():
            done = pos - 4 * lag
            for half in range(2):
                second_copy(done, 3, half).wait_recv()
            out_copy(done).start()

        for step in (3, 2, 1):

            @pl.when((pos >= step * lag) & (pos < chunks + step * lag))
            def _():
                second_step(pos - step * lag, step)

        @pl.when(pos < chunks)
        def _():
            wait(chunk_copies(pos), "chunk_wait")
            chunk, (row, lane), (row_high, lane_high) = chunk_place(pos)
            total = jnp.dot(
                hid[:, :LOW], pool[pl.ds(many(row, 128), LOW), pl.ds(many(lane, CHUNK), CHUNK)], preferred_element_type=F32
            ) + jnp.dot(
                hid[:, LOW:],
                pool[pl.ds(many(row_high, 128), ff - LOW), pl.ds(many(lane_high, CHUNK), CHUNK)],
                preferred_element_type=F32,
            )
            cols = pl.ds(many(chunk * CHUNK, CHUNK), CHUNK)
            part[:, cols] = total
            for half in range(2):
                away = pl.ds(many((1 - plan[half][2]) * (rows // 2), 16), rows // 2)
                some = pl.ds(many(chunk * CHUNK + half * side, side), side)
                st1[away, some] = part[away, some].astype(BF16)
                second_copy(pos, 0, half).start()

        return 0

    lax.fori_loop(0, chunks + 4 * lag, down_body, 0)

    def finish(pos, _):
        out_copy(pos).wait()
        for half in range(2):
            for step in range(4):
                second_copy(pos, step, half).wait_send()
        return 0

    lax.fori_loop(0, chunks, finish, 0)


def solution(mesh):
    def step(x, k_cache, v_cache, gain_a, wq, wo, gain_m, w_gate, w_up, w_down):
        rows, d = x.shape
        _, cache, kv_heads, head = k_cache.shape
        heads, ff = wq.shape[1] // head, w_gate.shape[1]
        keys, values = (t.transpose(0, 2, 3, 1).reshape(rows * kv_heads * head, cache) for t in (k_cache, v_cache))
        half = head // 2
        angle = np.float32(cache - 1) * np.float32(THETA) ** (-np.arange(half, dtype=np.float32) / np.float32(half))
        cos, sin = np.cos(angle.astype(np.float32)), np.sin(angle.astype(np.float32))
        turn = np.zeros((8, head), np.float32)
        turn[0], turn[1] = np.concatenate([cos, cos]), np.concatenate([-sin, sin])
        chunks = d // CHUNK
        dims = (rows, d, cache, heads, kv_heads, ff)
        dma = pltpu.SemaphoreType.DMA
        return pl.pallas_call(
            functools.partial(kernel, dims),
            out_shape=jax.ShapeDtypeStruct((rows, d), BF16),
            in_specs=[pl.BlockSpec(memory_space=pltpu.HBM)] * 11,
            out_specs=pl.BlockSpec(memory_space=pltpu.HBM),
            scratch_shapes=[
                pltpu.VMEM((UNITS * UNIT, WIDE), BF16),
                pltpu.VMEM((rows, d), BF16),
                pltpu.VMEM((d // 128, 128), BF16),
                pltpu.VMEM((d // 128, 128), BF16),
                pltpu.VMEM((8, head), F32),
                pltpu.VMEM((d // SLAB, rows, SLAB), BF16),
                pltpu.VMEM((-(-kv_heads * head // 128), rows * heads, 128), F32),
                pltpu.VMEM((-(-kv_heads * head // 128), rows * heads, 128), F32),
                pltpu.VMEM((rows, heads * head), BF16),
                pltpu.VMEM((rows, d), F32),
                pltpu.VMEM((rows, ff), F32),
                pltpu.VMEM((rows, d), BF16),
                pltpu.VMEM((rows, d // 2), BF16),
                pltpu.VMEM((rows, d // 4), BF16),
                pltpu.VMEM((rows, d // 4), BF16),
                pltpu.VMEM((rows, d), BF16),
                pltpu.VMEM((rows, d), BF16),
                pltpu.VMEM((rows, ff), BF16),
                pltpu.VMEM((chunks, 2, rows // 2, CHUNK // 2), BF16),
                pltpu.VMEM((chunks, 2, rows // 4, CHUNK // 2), BF16),
                pltpu.VMEM((chunks, 2, rows // 4, CHUNK // 2), BF16),
                dma((4,)),
                dma((d // UNIT,)),
                dma((RING, 2)),
                dma((3,)),
                dma((UNITS, 4)),
                dma((chunks, 2)),
                dma((chunks,)),
                dma((2, 4, 2)),
                dma((2, 4, 2)),
                dma((chunks, 4, 2)),
                dma((chunks, 4, 2)),
            ],
            compiler_params=pltpu.CompilerParams(
                collective_id=0, has_side_effects=True, vmem_limit_bytes=67043328
            ),
        )(x, keys, values, gain_a.reshape(d // 128, 128), wq, wo, gain_m.reshape(d // 128, 128), w_gate, w_up, w_down, turn)

    states, cache, columns, rows_of = P("dp", None), P("dp", None, "tp", None), P(None, "tp"), P("tp", None)
    return jax.shard_map(
        step,
        mesh=mesh,
        in_specs=(states, cache, cache, P(None), columns, rows_of, P(None), columns, columns, rows_of),
        out_specs=states,
        check_vma=False,
    )
```

```python
import functools

import jax
import jax.numpy as jnp
import numpy as np
from jax import lax
from jax.experimental import pallas as pl
from jax.experimental.pallas import tpu as pltpu
from jax.sharding import PartitionSpec as P

HEAD = 160
THETA = 10000
F32, BF16 = jnp.float32, jnp.bfloat16
MESH = pl.DeviceIdType.MESH

BATCH = 4
RING = 3
UNIT = 1280
UNITS = 10
WIDE = 2048
PITCH = 2048
BLOCK = 1024
HALVED = 3
SLAB = 640
CHUNK = 512
GROUPS = ((0, 8), (8, 12), (12, 16))
WO_AT = 6
LAG = 5


def many(v, n):
    return pl.multiple_of(v, n)


def kernel(dims, x_hbm, k_hbm, v_hbm, ga_hbm, wq_hbm, wo_hbm, gm_hbm, wg_hbm, wu_hbm, wd_hbm, turn_hbm, y_s, *scratch):
    rows, d, cache, heads, kv_heads, ff = dims
    (pool, x_s, ga_s, gm_s, turn_s, ab, qs, seen, part, accu, sent, sent2, got1, got2, got1b,
     misc_sem, wq_sem, kv_sem, wo_sem, slab_sem, wd_sem, a1_send, a1_recv0, a1_recv1, a2_send, a2_recv, a2_more) = scratch
    kvd = kv_heads * HEAD
    tiles = -(-kvd // 128)
    qd = heads * HEAD
    share = heads // kv_heads
    batches = rows // BATCH
    slabs = d // SLAB
    chunks = d // CHUNK
    places = UNITS * UNIT // (4 * SLAB)

    me = lax.axis_index("tp")
    beside = me + 1 - 2 * lax.rem(me, 2)
    across = 3 - me
    barrier = pltpu.get_barrier_semaphore()
    for other in (beside, across):
        pl.semaphore_signal(barrier, inc=1, device_id={"tp": other}, device_id_type=MESH)
    plan = ((beside, across), (across, beside))
    bits = ((lax.rem((me + 1) // 2, 2), me // 2), (me // 2, lax.rem(me, 2)))

    x_copy = pltpu.make_async_copy(x_hbm, x_s, misc_sem.at[0])
    ga_copy = pltpu.make_async_copy(ga_hbm, ga_s, misc_sem.at[1])
    gm_copy = pltpu.make_async_copy(gm_hbm, gm_s, misc_sem.at[2])
    turn_copy = pltpu.make_async_copy(turn_hbm, turn_s, misc_sem.at[3])

    def wq_copy(i):
        return pltpu.make_async_copy(
            wq_hbm.at[pl.ds(i * UNIT, UNIT)], pool.at[pl.ds((WO_AT + i) * UNIT, UNIT), pl.ds(0, qd)], wq_sem.at[i]
        )

    def kv_at(i):
        return many(lax.rem(i + 2, RING) * (2 * UNIT), UNIT)

    def kv_copies(i):
        slot = lax.rem(i + 2, RING)
        n = BATCH * kvd
        return [
            pltpu.make_async_copy(
                src.at[pl.ds(many(i * n, n), n)], pool.at[pl.ds(kv_at(i) + j * UNIT, n), pl.ds(0, WIDE)], kv_sem.at[slot]
            )
            for j, src in enumerate((k_hbm, v_hbm))
        ]

    def wo_copies():
        return [
            pltpu.make_async_copy(
                wo_hbm.at[:, pl.ds(j * WIDE, w)], pool.at[pl.ds((WO_AT + j) * UNIT, qd), pl.ds(0, w)], wo_sem.at[0]
            )
            for j, w in enumerate((WIDE, WIDE, d - 2 * WIDE))
        ]

    def slab_copies(k):
        place = lax.rem(k, places)
        copies = []
        for m, src in enumerate((wg_hbm, wu_hbm)):
            for j, w in enumerate((WIDE, ff - WIDE)):
                p = 2 * m + j
                copies.append(
                    pltpu.make_async_copy(
                        src.at[pl.ds(many(k * SLAB, SLAB), SLAB), pl.ds(j * WIDE, w)],
                        pool.at[pl.ds(many(place * (4 * SLAB), SLAB) + p * SLAB, SLAB), pl.ds(0, w)],
                        slab_sem.at[place],
                    )
                )
        return copies

    def start(copies):
        for c in copies:
            c.start(priority=1)

    def wait(copy, name):
        with jax.named_scope(name):
            copy.wait()

    def pool_wait(words, sem, name):
        n = words // WIDE
        if n * WIDE == words:
            region = pool.at[pl.ds(0, n), pl.ds(0, WIDE)]
        else:
            region = pool.at[pl.ds(0, words // CHUNK), pl.ds(0, CHUNK)]
        wait(pltpu.make_async_copy(region, region, sem), name)

    per_wide = WIDE // CHUNK

    def chunk_place(c):
        group = c // per_wide
        first = 6 * (1 - (group + 1) // 2) + 3 * (group // 2)
        return many(first * UNIT, UNIT), many(lax.rem(c, per_wide) * CHUNK, CHUNK)

    def chunk_copy(c):
        row, lane = chunk_place(c)
        return pltpu.make_async_copy(
            wd_hbm.at[:, pl.ds(many(c * CHUNK, CHUNK), CHUNK)], pool.at[pl.ds(row, ff), pl.ds(lane, CHUNK)], wd_sem.at[c]
        )

    x_copy.start()
    ga_copy.start()
    turn_copy.start()
    for i in range(d // UNIT):
        wq_copy(i).start(priority=1)
    for i in range(RING):
        start(kv_copies(i))
    gm_copy.start()

    @jax.named_scope("norm")
    def norm(src, gain_ref, row0, n):
        g = gain_ref[...].astype(F32)
        gain = jnp.concatenate([g[r : r + 1] for r in range(g.shape[0])], axis=1)

        def body(i, _):
            at = pl.ds(many(row0 + i * 16, 16), 16)
            wide = src[at, :].astype(F32)
            scale = lax.rsqrt(jnp.mean(wide * wide, -1, keepdims=True) + 1e-6)
            out = (wide * scale * gain).astype(BF16)
            for k in range(slabs):
                ab[k, at, :] = out[:, k * SLAB : (k + 1) * SLAB]
            return 0

        lax.fori_loop(0, n // 16, body, 0)

    wait(x_copy, "x_wait")
    wait(ga_copy, "ga_wait")
    norm(x_s, ga_s, 0, rows)

    per = UNIT // SLAB
    for i in range(d // UNIT):
        wait(wq_copy(i), "wq_wait")
        total = None
        for j in range(per):
            term = jnp.dot(
                ab[i * per + j], pool[(WO_AT + i) * UNIT + j * SLAB : (WO_AT + i) * UNIT + (j + 1) * SLAB, :qd],
                preferred_element_type=F32,
            )
            total = term if total is None else total + term
        part[:, :qd] = total if i == 0 else part[:, :qd] + total
    wait(turn_copy, "turn_wait")
    cos, sin = turn_s[0:1, :], turn_s[1:2, :]
    blank = jnp.zeros((rows, HEAD), F32)
    for j in range(heads):
        t = part[:, j * HEAD : (j + 1) * HEAD].astype(BF16).astype(F32)
        swapped = jnp.concatenate([t[:, HEAD // 2 :], t[:, : HEAD // 2]], axis=1)
        t = (t * cos + swapped * sin).astype(BF16).astype(F32)
        side = [blank] * kv_heads
        side[j // share] = t
        t = jnp.concatenate(side + [jnp.zeros((rows, tiles * 128 - kvd), F32)], axis=1)
        for c in range(tiles):
            qs[c, pl.ds(j, rows, stride=heads), :] = t[:, c * 128 : (c + 1) * 128]

    def swap(step, half, at, got, send_sem, recv_sem):
        return pltpu.make_async_remote_copy(
            src_ref=(sent, sent2)[step].at[at], dst_ref=got[step].at[at], send_sem=send_sem, recv_sem=recv_sem,
            device_id={"tp": plan[half][step]}, device_id_type=MESH,
        )

    def arrived(words, sem):
        region = sent.at[:, pl.ds(0, words // rows)]
        pltpu.make_async_copy(region, region, sem).wait()

    half_block = BLOCK // 2
    exposed = len(GROUPS) - 1

    def rows_of(g):
        b0, b1 = GROUPS[g]
        return b0 * BATCH, (b1 - b0) * BATCH

    def first_recv(g, step, c):
        return a1_recv1.at[step, c] if g == exposed else a1_recv0.at[step, g]

    def first_send(g, step, c):
        row0, n = rows_of(g)
        for half in range(2):
            at = (pl.ds(row0, n), pl.ds(many(c * BLOCK + half * half_block, half_block), half_block))
            swap(step, half, at, (got1, got2), a1_send.at[step], first_recv(g, step, c)).start()

    def first_step(g, step, c):
        row0, n = rows_of(g)
        at = (pl.ds(row0, n), pl.ds(many(c * BLOCK, BLOCK), BLOCK))
        if g == exposed:
            with jax.named_scope("first_wait"):
                arrived(n * BLOCK, first_recv(g, step, c))
        if step == 0:
            sent2[at] = (sent[at].astype(F32) + got1[at].astype(F32)).astype(BF16)
            first_send(g, 1, c)
        else:
            x_s[at] = (x_s[at].astype(F32) + (sent2[at].astype(F32) + got2[at].astype(F32))).astype(BF16)

    def all_blocks(g, step):
        row0, n = rows_of(g)
        with jax.named_scope("all_wait"):
            arrived(n * d, first_recv(g, step, 0))
        lax.fori_loop(0, d // BLOCK, lambda c, _: first_step(g, step, c) or 0, 0)

    @jax.named_scope("gather_seen")
    def gather_seen(g):
        row0, n = rows_of(g)
        for j in range(heads):
            o = jnp.concatenate([qs[c, pl.ds(row0 * heads + j, n, stride=heads), :] for c in range(tiles)], axis=1)
            h = j // share
            seen[row0 : row0 + n, j * HEAD : (j + 1) * HEAD] = o[:, h * HEAD : (h + 1) * HEAD].astype(BF16)

    @jax.named_scope("project")
    def project(g, c):
        row0, n = rows_of(g)
        row, lane = (WO_AT + c // 2) * UNIT, lax.rem(c, 2) * BLOCK
        w = pool[pl.ds(many(row, UNIT), qd), pl.ds(many(lane, BLOCK), BLOCK)]
        at = (slice(row0, row0 + n), pl.ds(many(c * BLOCK, BLOCK), BLOCK))
        sent[at] = jnp.dot(seen[row0 : row0 + n, :], w, preferred_element_type=F32).astype(BF16)
        first_send(g, 0, c)

    def attend(i, _):
        pool_wait(2 * BATCH * kvd * WIDE, kv_sem.at[lax.rem(i + 2, RING)], "kv_wait")
        at = kv_at(i)
        ws = []
        for j in range(BATCH):
            mine = pl.ds(many((i * BATCH + j) * heads, 8), heads)
            q = jnp.concatenate([qs[c, mine, :] for c in range(tiles)], axis=1)[:, :kvd].astype(BF16)
            scores = jnp.dot(q, pool[pl.ds(at + j * kvd, kvd), :WIDE], preferred_element_type=F32) * HEAD**-0.5
            top = jnp.max(scores, -1, keepdims=True)
            e = jnp.exp(scores - top)
            ws.append(e / jnp.sum(e, -1, keepdims=True))
        w = jnp.concatenate(ws, 0).astype(BF16)
        o = lax.dot_general(w, pool[pl.ds(at + UNIT, BATCH * kvd), :WIDE], (((1,), (1,)), ((), ())), preferred_element_type=F32)
        for j in range(BATCH):
            t = o[j * heads : (j + 1) * heads, j * kvd : (j + 1) * kvd]
            t = jnp.concatenate([t, jnp.zeros((heads, tiles * 128 - kvd), F32)], axis=1)
            for c in range(tiles):
                qs[c, pl.ds(many((i * BATCH + j) * heads, 8), heads), :] = t[:, c * 128 : (c + 1) * 128]

        @pl.when(i + RING < batches)
        def _():
            start(kv_copies(i + RING))

        @pl.when(i == 3)
        def _():
            start(wo_copies())

        @pl.when(i >= batches - RING)
        def _():
            start(slab_copies(i - (batches - RING)))

        end0, end1 = GROUPS[0][1], GROUPS[1][1]

        @pl.when(i == end0 - 1)
        def _():
            pool_wait(qd * d, wo_sem.at[0], "wo_wait")
            pl.semaphore_wait(barrier, 2)

        for g, end in enumerate((end0, end1)):

            @pl.when(i == end - 1)
            def _():
                gather_seen(g)
                lax.fori_loop(0, d // BLOCK, lambda c, _: project(g, c) or 0, 0)

            @pl.when(i == end + 2)
            def _():
                all_blocks(g, 0)

        @pl.when(i == end0 + 5)
        def _():
            all_blocks(0, 1)
            gm_copy.wait()
            norm(x_s, gm_s, *rows_of(0))

        return 0

    lax.fori_loop(0, batches, attend, 0)

    gather_seen(exposed)
    blocks = d // BLOCK

    def project_body(c, _):
        project(exposed, c)

        @pl.when(c == blocks - 1)
        def _():
            for k in range(RING, places):
                start(slab_copies(k))

        return 0

    lax.fori_loop(0, blocks, project_body, 0)
    all_blocks(exposed - 1, 1)
    norm(x_s, gm_s, *rows_of(exposed - 1))
    accu[...] = jnp.zeros_like(accu)
    part[:, :ff] = jnp.zeros((rows, ff), F32)
    for step in range(2):
        lax.fori_loop(0, blocks, lambda c, _: first_step(exposed, step, c) or 0, 0)
    norm(x_s, gm_s, *rows_of(exposed))
    for step in range(2):
        arrived(rows * d, a1_send.at[step])

    def slab_body(k, _):
        place = lax.rem(k, places)
        pool_wait(2 * SLAB * ff, slab_sem.at[place], "slab_wait")
        lhs = ab[k]
        for m, acc in enumerate((part, accu)):
            for j, w in enumerate((WIDE, ff - WIDE)):
                at = pl.ds(many(place * (4 * SLAB), SLAB) + (2 * m + j) * SLAB, SLAB)
                acc[:, j * WIDE : j * WIDE + w] += jnp.dot(lhs, pool[at, :w], preferred_element_type=F32)

        @pl.when(k < slabs - places)
        def _():
            start(slab_copies(k + places))

        for after, first, last in ((4, 0, per_wide), (6, per_wide, 2 * per_wide), (7, 2 * per_wide, chunks)):

            @pl.when(k == after)
            def _():
                for c in range(first, last):
                    start([chunk_copy(c)])

        return 0

    lax.fori_loop(0, slabs, slab_body, 0)

    def hidden_body(c, _):
        at = pl.ds(many(c * 384, 128), 384)
        got1[:, at] = (jax.nn.silu(part[:, at]) * accu[:, at]).astype(BF16)
        return 0

    lax.fori_loop(0, ff // 384, hidden_body, 0)

    side = CHUNK // 2
    row2, row4 = rows // 2, rows // 4

    def columns_of(c, half):
        return pl.ds(many(c * CHUNK + half * side, side), side)

    def chunk_recv(c, step):
        return a2_recv.at[c, step] if step < 2 else a2_more.at[c, step - 2]

    def full_send(c, step):
        for half in range(2):
            at = (slice(None), columns_of(c, half))
            swap(step, half, at, (got1b, y_s), a2_send.at[step], chunk_recv(c, step)).start()

    @jax.named_scope("full_step")
    def full_step(c, step):
        arrived(rows * CHUNK, chunk_recv(c, step))
        at = (slice(None), pl.ds(many(c * CHUNK, CHUNK), CHUNK))
        if step == 0:
            sent2[at] = (sent[at].astype(F32) + got1b[at].astype(F32)).astype(BF16)
            full_send(c, 1)
        else:
            y_s[at] = (x_s[at].astype(F32) + (sent2[at].astype(F32) + y_s[at].astype(F32))).astype(BF16)

    def halved_send(c, step, half):
        bit1, bit2 = bits[half]
        row, n, src, dst, to = (
            ((1 - bit1) * row2, row2, sent, got1b, 0),
            (bit1 * row2 + (1 - bit2) * row4, row4, sent2, y_s, 1),
            (bit1 * row2 + bit2 * row4, row4, y_s, y_s, 1),
            (bit1 * row2, row2, y_s, y_s, 0),
        )[step]
        at = (pl.ds(many(row, 16), n), columns_of(c, half))
        pltpu.make_async_remote_copy(
            src_ref=src.at[at], dst_ref=dst.at[at], send_sem=a2_send.at[step], recv_sem=chunk_recv(c, step),
            device_id={"tp": plan[half][to]}, device_id_type=MESH,
        ).start()

    @jax.named_scope("halved_step")
    def halved_step(c, step):
        arrived((row2, row4, row4, row2)[step] * CHUNK, chunk_recv(c, step))
        for half in range(2):
            bit1, bit2 = bits[half]
            cols = columns_of(c, half)
            if step == 0:
                at = (pl.ds(many(bit1 * row2 + (1 - bit2) * row4, 16), row4), cols)
                sent2[at] = (part[at] + got1b[at].astype(F32)).astype(BF16)
            elif step == 1:
                at = (pl.ds(many(bit1 * row2 + bit2 * row4, 16), row4), cols)
                y_s[at] = (
                    x_s[at].astype(F32) + (part[at] + got1b[at].astype(F32) + y_s[at].astype(F32))
                ).astype(BF16)
            if step < 3:
                halved_send(c, step + 1, half)

    def down(i):
        wait(chunk_copy(i), "chunk_wait")
        row, lane = chunk_place(i)
        return jnp.dot(got1[:, :ff], pool[pl.ds(row, ff), pl.ds(lane, CHUNK)], preferred_element_type=F32)

    def down_body(i, _):
        for step in (3, 2, 1, 0):
            at = (step + 1) * LAG

            @pl.when((i >= at) & (i < HALVED + at))
            def _():
                halved_step(i - at, step)

            if step < 2:

                @pl.when((i >= HALVED + at) & (i < chunks + at))
                def _():
                    full_step(i - at, step)

        @pl.when(i < HALVED)
        def _():
            cols = pl.ds(many(i * CHUNK, CHUNK), CHUNK)
            part[:, cols] = down(i)
            for half in range(2):
                at = (pl.ds(many((1 - bits[half][0]) * row2, 16), row2), columns_of(i, half))
                sent[at] = part[at].astype(BF16)
                halved_send(i, 0, half)

        @pl.when((i >= HALVED) & (i < chunks))
        def _():
            sent[:, pl.ds(many(i * CHUNK, CHUNK), CHUNK)] = down(i).astype(BF16)
            full_send(i, 0)

        return 0

    lax.fori_loop(0, max(chunks + 2 * LAG, HALVED + 4 * LAG), down_body, 0)
    whole = chunks - HALVED
    for step, n in enumerate((HALVED * row2 + whole * rows, HALVED * row4 + whole * rows, HALVED * row4, HALVED * row2)):
        arrived(n * CHUNK, a2_send.at[step])


def solution(mesh):
    def step(x, k_cache, v_cache, gain_a, wq, wo, gain_m, w_gate, w_up, w_down):
        rows, d = x.shape
        _, cache, kv_heads, head = k_cache.shape
        heads, ff = wq.shape[1] // head, w_gate.shape[1]
        keys, values = (t.transpose(0, 2, 3, 1).reshape(rows * kv_heads * head, cache) for t in (k_cache, v_cache))
        half = head // 2
        angle = np.float32(cache - 1) * np.float32(THETA) ** (-np.arange(half, dtype=np.float32) / np.float32(half))
        cos, sin = np.cos(angle.astype(np.float32)), np.sin(angle.astype(np.float32))
        turn = np.zeros((8, head), np.float32)
        turn[0], turn[1] = np.concatenate([cos, cos]), np.concatenate([-sin, sin])
        chunks = d // CHUNK
        dims = (rows, d, cache, heads, kv_heads, ff)
        dma = pltpu.SemaphoreType.DMA
        return pl.pallas_call(
            functools.partial(kernel, dims),
            out_shape=pltpu.VMEM((rows, d), BF16),
            in_specs=[pl.BlockSpec(memory_space=pltpu.HBM)] * 11,
            out_specs=pl.BlockSpec(memory_space=pltpu.VMEM),
            scratch_shapes=[
                pltpu.VMEM((UNITS * UNIT, PITCH), BF16),
                pltpu.VMEM((rows, d), BF16),
                pltpu.VMEM((d // 128, 128), BF16),
                pltpu.VMEM((d // 128, 128), BF16),
                pltpu.VMEM((8, head), F32),
                pltpu.VMEM((d // SLAB, rows, SLAB), BF16),
                pltpu.VMEM((-(-kv_heads * head // 128), rows * heads, 128), F32),
                pltpu.VMEM((rows, heads * head), BF16),
                pltpu.VMEM((rows, d), F32),
                pltpu.VMEM((rows, ff), F32),
                pltpu.VMEM((rows, d), BF16),
                pltpu.VMEM((rows, d), BF16),
                pltpu.VMEM((rows, d), BF16),
                pltpu.VMEM((rows, d), BF16),
                pltpu.VMEM((rows, d), BF16),
                dma((4,)),
                dma((d // UNIT,)),
                dma((RING,)),
                dma((1,)),
                dma((UNITS * UNIT // (4 * SLAB),)),
                dma((chunks,)),
                dma((2,)),
                dma((2, len(GROUPS) - 1)),
                dma((2, d // BLOCK)),
                dma((4,)),
                dma((chunks, 2)),
                dma((HALVED, 2)),
            ],
            compiler_params=pltpu.CompilerParams(
                collective_id=0, has_side_effects=True, vmem_limit_bytes=66350000
            ),
        )(x, keys, values, gain_a.reshape(d // 128, 128), wq, wo, gain_m.reshape(d // 128, 128), w_gate, w_up, w_down, turn)

    states, cache, columns, rows_of = P("dp", None), P("dp", None, "tp", None), P(None, "tp"), P("tp", None)
    return jax.shard_map(
        step,
        mesh=mesh,
        in_specs=(states, cache, cache, P(None), columns, rows_of, P(None), columns, columns, rows_of),
        out_specs=states,
        check_vma=False,
    )
```

```python
import functools

import jax
import jax.numpy as jnp
import numpy as np
from jax import lax
from jax.experimental import pallas as pl
from jax.experimental.pallas import tpu as pltpu
from jax.sharding import PartitionSpec as P

HEAD = 160
THETA = 10000
F32, BF16 = jnp.float32, jnp.bfloat16
MESH = pl.DeviceIdType.MESH

BATCH = 4
RING = 3
UNIT = 1280
UNITS = 10
WIDE = 2048
PITCH = 2048
BLOCK = 1024
SLAB = 640
CHUNK = 512
GROUPS = ((0, 12), (12, 16))
WO_AT = 6
EARLY = 3
WO_SEM = 4
HALVED = 6
LAG = 5


def many(v, n):
    return pl.multiple_of(v, n)


def kernel(dims, x_hbm, k_hbm, v_hbm, ga_hbm, wq_hbm, wo_hbm, gm_hbm, wg_hbm, wu_hbm, wd_hbm, turn_hbm, y_s, *scratch):
    rows, d, cache, heads, kv_heads, ff = dims
    (pool, x_s, ga_s, gm_s, turn_s, ab, qs, seen, part, accu, sent, sent2, got1, got2, got1b,
     misc_sem, flow, kv_sem, a1_send, a1_recv0, a1_recv1, a2_send, a2_recv, a2_back) = scratch
    kvd = kv_heads * HEAD
    tiles = -(-kvd // 128)
    qd = heads * HEAD
    share = heads // kv_heads
    batches = rows // BATCH
    slabs = d // SLAB
    chunks = d // CHUNK
    places = UNITS * UNIT // (4 * SLAB)

    me = lax.axis_index("tp")
    beside = me + 1 - 2 * lax.rem(me, 2)
    across = 3 - me
    barrier = pltpu.get_barrier_semaphore()
    for other in (beside, across):
        pl.semaphore_signal(barrier, inc=1, device_id={"tp": other}, device_id_type=MESH)
    plan = ((beside, across), (across, beside))
    kept = (lax.rem((me + 1) // 2, 2), me // 2)


    x_copy = pltpu.make_async_copy(x_hbm, x_s, misc_sem.at[0])
    ga_copy = pltpu.make_async_copy(ga_hbm, ga_s, misc_sem.at[1])
    gm_copy = pltpu.make_async_copy(gm_hbm, gm_s, misc_sem.at[2])
    turn_copy = pltpu.make_async_copy(turn_hbm, turn_s, misc_sem.at[3])

    def wq_copy(i):
        return pltpu.make_async_copy(
            wq_hbm.at[pl.ds(i * UNIT, UNIT)], pool.at[pl.ds((WO_AT + i) * UNIT, UNIT), pl.ds(0, qd)], flow.at[i]
        )

    def kv_at(i):
        return many(lax.rem(i + 2, RING) * (2 * UNIT), UNIT)

    def kv_copies(i):
        slot = lax.rem(i + 2, RING)
        n = BATCH * kvd
        return [
            pltpu.make_async_copy(
                src.at[pl.ds(many(i * n, n), n)], pool.at[pl.ds(kv_at(i) + j * UNIT, n), pl.ds(0, WIDE)], kv_sem.at[slot, j]
            )
            for j, src in enumerate((k_hbm, v_hbm))
        ]

    def wo_copies():
        return [
            pltpu.make_async_copy(
                wo_hbm.at[:, pl.ds(j * WIDE, w)], pool.at[pl.ds((WO_AT + j) * UNIT, qd), pl.ds(0, w)], flow.at[WO_SEM]
            )
            for j, w in enumerate((WIDE, WIDE, d - 2 * WIDE))
        ]

    def slab_sem(place):
        return flow.at[WO_SEM + 1 + lax.rem(place + 2, places)]

    def slab_copies(k):
        place = lax.rem(k, places)
        copies = []
        for m, src in enumerate((wg_hbm, wu_hbm)):
            for j, w in enumerate((WIDE, ff - WIDE)):
                p = 2 * m + j
                copies.append(
                    pltpu.make_async_copy(
                        src.at[pl.ds(many(k * SLAB, SLAB), SLAB), pl.ds(j * WIDE, w)],
                        pool.at[pl.ds(many(place * (4 * SLAB), SLAB) + p * SLAB, SLAB), pl.ds(0, w)],
                        slab_sem(place),
                    )
                )
        return copies

    def start(copies):
        for c in copies:
            c.start(priority=1)

    def wait(copy, name):
        with jax.named_scope(name):
            copy.wait()

    def pool_wait(words, sem, name):
        n = words // WIDE
        if n * WIDE == words:
            region = pool.at[pl.ds(0, n), pl.ds(0, WIDE)]
        else:
            region = pool.at[pl.ds(0, words // CHUNK), pl.ds(0, CHUNK)]
        wait(pltpu.make_async_copy(region, region, sem), name)

    per_wide = WIDE // CHUNK

    def chunk_place(c):
        group = c // per_wide
        first = 6 * (1 - (group + 1) // 2) + 3 * (group // 2)
        return many(first * UNIT, UNIT), many(lax.rem(c, per_wide) * CHUNK, CHUNK)

    def chunk_copy(c):
        row, lane = chunk_place(c)
        return pltpu.make_async_copy(
            wd_hbm.at[:, pl.ds(many(c * CHUNK, CHUNK), CHUNK)], pool.at[pl.ds(row, ff), pl.ds(lane, CHUNK)], flow.at[c]
        )

    x_copy.start()
    ga_copy.start()
    turn_copy.start()
    for i in range(d // UNIT):
        wq_copy(i).start(priority=1)
    for i in range(RING):
        start(kv_copies(i))
    gm_copy.start()

    @jax.named_scope("norm")
    def norm(src, gain_ref, row0, n):
        g = gain_ref[...].astype(F32)
        gain = jnp.concatenate([g[r : r + 1] for r in range(g.shape[0])], axis=1)

        def body(i, _):
            at = pl.ds(many(row0 + i * 16, 16), 16)
            wide = src[at, :].astype(F32)
            scale = lax.rsqrt(jnp.mean(wide * wide, -1, keepdims=True) + 1e-6)
            out = (wide * scale * gain).astype(BF16)
            for k in range(slabs):
                ab[k, at, :] = out[:, k * SLAB : (k + 1) * SLAB]
            return 0

        lax.fori_loop(0, n // 16, body, 0)

    wait(x_copy, "x_wait")
    wait(ga_copy, "ga_wait")
    norm(x_s, ga_s, 0, rows)

    per = UNIT // SLAB
    for i in range(d // UNIT):
        wait(wq_copy(i), "wq_wait")
        total = None
        for j in range(per):
            term = jnp.dot(
                ab[i * per + j], pool[(WO_AT + i) * UNIT + j * SLAB : (WO_AT + i) * UNIT + (j + 1) * SLAB, :qd],
                preferred_element_type=F32,
            )
            total = term if total is None else total + term
        part[:, :qd] = total if i == 0 else part[:, :qd] + total
    wait(turn_copy, "turn_wait")
    cos, sin = turn_s[0:1, :], turn_s[1:2, :]
    blank = jnp.zeros((rows, HEAD), F32)
    for j in range(heads):
        t = part[:, j * HEAD : (j + 1) * HEAD].astype(BF16).astype(F32)
        swapped = jnp.concatenate([t[:, HEAD // 2 :], t[:, : HEAD // 2]], axis=1)
        t = (t * cos + swapped * sin).astype(BF16).astype(F32)
        side = [blank] * kv_heads
        side[j // share] = t
        t = jnp.concatenate(side + [jnp.zeros((rows, tiles * 128 - kvd), F32)], axis=1)
        for c in range(tiles):
            qs[c, pl.ds(j, rows, stride=heads), :] = t[:, c * 128 : (c + 1) * 128]

    def swap(step, half, at, got, send_sem, recv_sem):
        return pltpu.make_async_remote_copy(
            src_ref=(sent, sent2)[step].at[at], dst_ref=got[step].at[at], send_sem=send_sem, recv_sem=recv_sem,
            device_id={"tp": plan[half][step]}, device_id_type=MESH,
        )

    def arrived(words, sem):
        region = sent.at[:, pl.ds(0, words // rows)]
        pltpu.make_async_copy(region, region, sem).wait()

    half_block = BLOCK // 2
    exposed = len(GROUPS) - 1

    def rows_of(g):
        b0, b1 = GROUPS[g]
        return b0 * BATCH, (b1 - b0) * BATCH

    def first_recv(g, step, c):
        return a1_recv1.at[step, c] if g == exposed else a1_recv0.at[step, g]

    def first_send(g, step, c):
        row0, n = rows_of(g)
        for half in range(2):
            at = (pl.ds(row0, n), pl.ds(many(c * BLOCK + half * half_block, half_block), half_block))
            swap(step, half, at, (got1, got2), a1_send.at[step], first_recv(g, step, c)).start()

    def first_step(g, step, c):
        row0, n = rows_of(g)
        at = (pl.ds(row0, n), pl.ds(many(c * BLOCK, BLOCK), BLOCK))
        if g == exposed:
            with jax.named_scope("first_wait"):
                arrived(n * BLOCK, first_recv(g, step, c))
        if step == 0:
            sent2[at] = (sent[at].astype(F32) + got1[at].astype(F32)).astype(BF16)
            first_send(g, 1, c)
        else:
            x_s[at] = (x_s[at].astype(F32) + (sent2[at].astype(F32) + got2[at].astype(F32))).astype(BF16)

    def all_blocks(g, step):
        row0, n = rows_of(g)
        with jax.named_scope("all_wait"):
            arrived(n * d, first_recv(g, step, 0))
        lax.fori_loop(0, d // BLOCK, lambda c, _: first_step(g, step, c) or 0, 0)

    @jax.named_scope("gather_seen")
    def gather_seen(g):
        row0, n = rows_of(g)
        for j in range(heads):
            o = jnp.concatenate([qs[c, pl.ds(row0 * heads + j, n, stride=heads), :] for c in range(tiles)], axis=1)
            h = j // share
            seen[row0 : row0 + n, j * HEAD : (j + 1) * HEAD] = o[:, h * HEAD : (h + 1) * HEAD].astype(BF16)

    @jax.named_scope("project")
    def project(g, c):
        row0, n = rows_of(g)
        row, lane = (WO_AT + c // 2) * UNIT, lax.rem(c, 2) * BLOCK
        w = pool[pl.ds(many(row, UNIT), qd), pl.ds(many(lane, BLOCK), BLOCK)]
        at = (slice(row0, row0 + n), pl.ds(many(c * BLOCK, BLOCK), BLOCK))
        sent[at] = jnp.dot(seen[row0 : row0 + n, :], w, preferred_element_type=F32).astype(BF16)
        first_send(g, 0, c)

    def attend(i, early):
        slot = lax.rem(i + 2, RING)

        def kv_wait(j, name):
            pool_wait(BATCH * kvd * WIDE, kv_sem.at[slot, j], name)

        kv_wait(0, "k_wait")
        if not early:
            kv_wait(1, "v_wait")
        at = kv_at(i)
        ws = []
        for j in range(BATCH):
            mine = pl.ds(many((i * BATCH + j) * heads, 8), heads)
            q = jnp.concatenate([qs[c, mine, :] for c in range(tiles)], axis=1)[:, :kvd].astype(BF16)
            scores = jnp.dot(q, pool[pl.ds(at + j * kvd, kvd), :WIDE], preferred_element_type=F32) * HEAD**-0.5
            top = jnp.max(scores, -1, keepdims=True)
            e = jnp.exp(scores - top)
            ws.append(e / jnp.sum(e, -1, keepdims=True))
        w = jnp.concatenate(ws, 0).astype(BF16)
        if early:
            kv_wait(1, "v_wait")
        o = lax.dot_general(w, pool[pl.ds(at + UNIT, BATCH * kvd), :WIDE], (((1,), (1,)), ((), ())), preferred_element_type=F32)
        for j in range(BATCH):
            t = o[j * heads : (j + 1) * heads, j * kvd : (j + 1) * kvd]
            t = jnp.concatenate([t, jnp.zeros((heads, tiles * 128 - kvd), F32)], axis=1)
            for c in range(tiles):
                qs[c, pl.ds(many((i * BATCH + j) * heads, 8), heads), :] = t[:, c * 128 : (c + 1) * 128]

        @pl.when(i + RING < batches)
        def _():
            start(kv_copies(i + RING))

        @pl.when(i == 6)
        def _():
            start(wo_copies())

        @pl.when(i >= batches - RING)
        def _():
            start(slab_copies(i - (batches - RING)))

        end0 = GROUPS[0][1]

        @pl.when(i == end0 - 1)
        def _():
            pool_wait(qd * d, flow.at[WO_SEM], "wo_wait")
            pl.semaphore_wait(barrier, 2)
            gather_seen(0)
            lax.fori_loop(0, d // BLOCK, lambda c, _: project(0, c) or 0, 0)

        @pl.when(i == end0 + 1)
        def _():
            all_blocks(0, 0)

        return 0

    lax.fori_loop(0, GROUPS[0][1], lambda i, _: attend(i, True), 0)
    lax.fori_loop(GROUPS[0][1], batches, lambda i, _: attend(i, False), 0)

    gather_seen(exposed)
    blocks = d // BLOCK

    def project_body(c, _):
        project(exposed, c)

        @pl.when(c == blocks - 1)
        def _():
            for k in range(RING, places):
                start(slab_copies(k))

        return 0

    lax.fori_loop(0, blocks, project_body, 0)
    all_blocks(exposed - 1, 1)
    gm_copy.wait()
    norm(x_s, gm_s, *rows_of(exposed - 1))
    accu[...] = jnp.zeros_like(accu)
    part[:, :ff] = jnp.zeros((rows, ff), F32)

    @jax.named_scope("slab")
    def slab_dots(k, row0, n):
        place = lax.rem(k, places)
        mine = slice(row0, row0 + n)
        lhs = ab[k, mine, :]
        for m, acc in enumerate((part, accu)):
            for j, w in enumerate((WIDE, ff - WIDE)):
                at = pl.ds(many(place * (4 * SLAB), SLAB) + (2 * m + j) * SLAB, SLAB)
                acc[mine, j * WIDE : j * WIDE + w] += jnp.dot(lhs, pool[at, :w], preferred_element_type=F32)

    def slab_wait(k):
        pool_wait(2 * SLAB * ff, slab_sem(lax.rem(k, places)), "slab_wait")

    def refill(k):
        @pl.when(k < slabs - places)
        def _():
            start(slab_copies(k + places))

        for after, first, last in ((4, 0, per_wide), (6, per_wide, 2 * per_wide), (7, 2 * per_wide, chunks)):

            @pl.when(k == after)
            def _():
                for c in range(first, last):
                    start([chunk_copy(c)])

    last_row, last_rows = rows_of(exposed)

    def early_body(k, _):
        slab_wait(k)
        slab_dots(k, 0, last_row)

        @pl.when(k == 0)
        def _():
            lax.fori_loop(0, blocks, lambda c, _: first_step(exposed, 0, c) or 0, 0)

        return 0

    lax.fori_loop(0, EARLY, early_body, 0)
    lax.fori_loop(0, blocks, lambda c, _: first_step(exposed, 1, c) or 0, 0)
    norm(x_s, gm_s, last_row, last_rows)
    for step in range(2):
        arrived(rows * d, a1_send.at[step])

    def late_body(k, _):
        slab_dots(k, last_row, last_rows)
        refill(k)
        return 0

    lax.fori_loop(0, EARLY, late_body, 0)

    def slab_body(k, _):
        slab_wait(k)
        slab_dots(k, 0, rows)
        refill(k)
        return 0

    lax.fori_loop(EARLY, slabs, slab_body, 0)

    def hidden_body(c, _):
        at = pl.ds(many(c * 384, 128), 384)
        got1[:, at] = (jax.nn.silu(part[:, at]) * accu[:, at]).astype(BF16)
        return 0

    lax.fori_loop(0, ff // 384, hidden_body, 0)

    side = CHUNK // 2

    def columns_of(c, half):
        return pl.ds(many(c * CHUNK + half * side, side), side)

    def full_send(c, step):
        for half in range(2):
            at = (slice(None), columns_of(c, half))
            swap(step, half, at, (got1b, y_s), a2_send.at[step], a2_recv.at[c, step]).start()

    @jax.named_scope("full_step")
    def full_step(c, step):
        arrived(rows * CHUNK, a2_recv.at[c, step])
        at = (slice(None), pl.ds(many(c * CHUNK, CHUNK), CHUNK))
        if step == 0:
            sent2[at] = (sent[at].astype(F32) + got1b[at].astype(F32)).astype(BF16)
            full_send(c, 1)
        else:
            y_s[at] = (x_s[at].astype(F32) + (sent2[at].astype(F32) + y_s[at].astype(F32))).astype(BF16)

    row2 = rows // 2

    def halved_send(c, step):
        for half in range(2):
            row = (1 - kept[half]) * row2 if step == 0 else kept[half] * row2
            at = (pl.ds(many(row, 32), row2), columns_of(c, half))
            pltpu.make_async_remote_copy(
                src_ref=(sent, sent2, y_s)[step].at[at], dst_ref=(got1b, y_s, y_s)[step].at[at], send_sem=a2_send.at[step],
                recv_sem=a2_back.at[c] if step == 2 else a2_recv.at[c, step],
                device_id={"tp": plan[half][step % 2]}, device_id_type=MESH,
            ).start()

    @jax.named_scope("halved_step")
    def halved_step(c, step):
        arrived(row2 * CHUNK, a2_back.at[c] if step == 2 else a2_recv.at[c, step])
        if step == 2:
            return
        for half in range(2):
            at = (pl.ds(many(kept[half] * row2, 32), row2), columns_of(c, half))
            if step == 0:
                sent2[at] = (part[at] + got1b[at].astype(F32)).astype(BF16)
            else:
                y_s[at] = (x_s[at].astype(F32) + (sent2[at].astype(F32) + y_s[at].astype(F32))).astype(BF16)
        halved_send(c, step + 1)

    def down(i):
        wait(chunk_copy(i), "chunk_wait")
        row, lane = chunk_place(i)
        return jnp.dot(got1[:, :ff], pool[pl.ds(row, ff), pl.ds(lane, CHUNK)], preferred_element_type=F32)

    def down_body(i, _):
        for step in (2, 1, 0):
            at = (step + 1) * LAG

            @pl.when((i >= at) & (i < HALVED + at))
            def _():
                halved_step(i - at, step)

            if step < 2:

                @pl.when((i >= HALVED + at) & (i < chunks + at))
                def _():
                    full_step(i - at, step)

        @pl.when(i < HALVED)
        def _():
            part[:, pl.ds(many(i * CHUNK, CHUNK), CHUNK)] = down(i)
            for half in range(2):
                at = (pl.ds(many((1 - kept[half]) * row2, 32), row2), columns_of(i, half))
                sent[at] = part[at].astype(BF16)
            halved_send(i, 0)

        @pl.when((i >= HALVED) & (i < chunks))
        def _():
            sent[:, pl.ds(many(i * CHUNK, CHUNK), CHUNK)] = down(i).astype(BF16)
            full_send(i, 0)

        return 0

    lax.fori_loop(0, max(chunks + 2 * LAG, HALVED + 3 * LAG), down_body, 0)
    whole = chunks - HALVED
    for step, n in enumerate((HALVED * row2 + whole * rows, HALVED * row2 + whole * rows, HALVED * row2)):
        arrived(n * CHUNK, a2_send.at[step])


def solution(mesh):
    def step(x, k_cache, v_cache, gain_a, wq, wo, gain_m, w_gate, w_up, w_down):
        rows, d = x.shape
        _, cache, kv_heads, head = k_cache.shape
        heads, ff = wq.shape[1] // head, w_gate.shape[1]
        keys, values = (t.transpose(0, 2, 3, 1).reshape(rows * kv_heads * head, cache) for t in (k_cache, v_cache))
        half = head // 2
        angle = np.float32(cache - 1) * np.float32(THETA) ** (-np.arange(half, dtype=np.float32) / np.float32(half))
        cos, sin = np.cos(angle.astype(np.float32)), np.sin(angle.astype(np.float32))
        turn = np.zeros((8, head), np.float32)
        turn[0], turn[1] = np.concatenate([cos, cos]), np.concatenate([-sin, sin])
        chunks = d // CHUNK
        dims = (rows, d, cache, heads, kv_heads, ff)
        dma = pltpu.SemaphoreType.DMA
        return pl.pallas_call(
            functools.partial(kernel, dims),
            out_shape=pltpu.VMEM((rows, d), BF16),
            in_specs=[pl.BlockSpec(memory_space=pltpu.HBM)] * 11,
            out_specs=pl.BlockSpec(memory_space=pltpu.VMEM),
            scratch_shapes=[
                pltpu.VMEM((UNITS * UNIT, PITCH), BF16),
                pltpu.VMEM((rows, d), BF16),
                pltpu.VMEM((d // 128, 128), BF16),
                pltpu.VMEM((d // 128, 128), BF16),
                pltpu.VMEM((8, head), F32),
                pltpu.VMEM((d // SLAB, rows, SLAB), BF16),
                pltpu.VMEM((-(-kv_heads * head // 128), rows * heads, 128), F32),
                pltpu.VMEM((rows, heads * head), BF16),
                pltpu.VMEM((rows, d), F32),
                pltpu.VMEM((rows, ff), F32),
                pltpu.VMEM((rows, d), BF16),
                pltpu.VMEM((rows, d), BF16),
                pltpu.VMEM((rows, d), BF16),
                pltpu.VMEM((rows, d), BF16),
                pltpu.VMEM((rows, d), BF16),
                dma((4,)),
                dma((chunks,)),
                dma((RING, 2)),
                dma((2,)),
                dma((2, len(GROUPS) - 1)),
                dma((2, d // BLOCK)),
                dma((3,)),
                dma((chunks, 2)),
                dma((HALVED,)),
            ],
            compiler_params=pltpu.CompilerParams(
                collective_id=0, has_side_effects=True, vmem_limit_bytes=66350000
            ),
        )(x, keys, values, gain_a.reshape(d // 128, 128), wq, wo, gain_m.reshape(d // 128, 128), w_gate, w_up, w_down, turn)

    states, cache, columns, rows_of = P("dp", None), P("dp", None, "tp", None), P(None, "tp"), P("tp", None)
    return jax.shard_map(
        step,
        mesh=mesh,
        in_specs=(states, cache, cache, P(None), columns, rows_of, P(None), columns, columns, rows_of),
        out_specs=states,
        check_vma=False,
    )
```

```python
import functools

import jax
import jax.numpy as jnp
import numpy as np
from jax import lax
from jax.experimental import pallas as pl
from jax.experimental.pallas import tpu as pltpu
from jax.sharding import PartitionSpec as P

HEAD = 160
THETA = 10000
F32, BF16 = jnp.float32, jnp.bfloat16
MESH = pl.DeviceIdType.MESH

BATCH = 4
RING = 3
UNIT = 1280
UNITS = 10
WIDE = 2048
PITCH = 2048
BLOCK = 1024
SLAB = 640
CHUNK = 512
GROUPS = ((0, 12), (12, 16))
WO_AT = 6
EARLY = 3
WO_SEM = 4
HALVED = 6
LAG = 5


def many(v, n):
    return pl.multiple_of(v, n)


def kernel(dims, x_hbm, k_hbm, v_hbm, ga_hbm, wq_hbm, wo_hbm, gm_hbm, wg_hbm, wu_hbm, wd_hbm, turn_hbm, y_s, *scratch):
    rows, d, cache, heads, kv_heads, ff = dims
    (pool, x_s, ga_s, gm_s, turn_s, ab, qs, seen, part, accu, sent, sent2, got1, got2, got1b,
     misc_sem, flow, kv_sem, a1_send, a1_recv0, a1_recv1, a2_send, a2_recv, a2_back) = scratch
    kvd = kv_heads * HEAD
    tiles = -(-kvd // 128)
    qd = heads * HEAD
    share = heads // kv_heads
    batches = rows // BATCH
    slabs = d // SLAB
    chunks = d // CHUNK
    places = UNITS * UNIT // (4 * SLAB)

    me = lax.axis_index("tp")
    beside = me + 1 - 2 * lax.rem(me, 2)
    across = 3 - me
    barrier = pltpu.get_barrier_semaphore()
    for other in (beside, across):
        pl.semaphore_signal(barrier, inc=1, device_id={"tp": other}, device_id_type=MESH)
    plan = ((beside, across), (across, beside))
    kept = (lax.rem((me + 1) // 2, 2), me // 2)


    x_copy = pltpu.make_async_copy(x_hbm, x_s, misc_sem.at[0])
    ga_copy = pltpu.make_async_copy(ga_hbm, ga_s, misc_sem.at[1])
    gm_copy = pltpu.make_async_copy(gm_hbm, gm_s, misc_sem.at[2])
    turn_copy = pltpu.make_async_copy(turn_hbm, turn_s, misc_sem.at[3])

    def wq_copy(i):
        return pltpu.make_async_copy(
            wq_hbm.at[pl.ds(i * UNIT, UNIT)], pool.at[pl.ds((WO_AT + i) * UNIT, UNIT), pl.ds(0, qd)], flow.at[i]
        )

    def kv_at(i):
        return many(lax.rem(i + 2, RING) * (2 * UNIT), UNIT)

    def kv_copies(i):
        slot = lax.rem(i + 2, RING)
        n = BATCH * kvd
        return [
            pltpu.make_async_copy(
                src.at[pl.ds(many(i * n, n), n)], pool.at[pl.ds(kv_at(i) + j * UNIT, n), pl.ds(0, WIDE)], kv_sem.at[slot, j]
            )
            for j, src in enumerate((k_hbm, v_hbm))
        ]

    def wo_copies():
        return [
            pltpu.make_async_copy(
                wo_hbm.at[:, pl.ds(j * WIDE, w)], pool.at[pl.ds((WO_AT + j) * UNIT, qd), pl.ds(0, w)], flow.at[WO_SEM]
            )
            for j, w in enumerate((WIDE, WIDE, d - 2 * WIDE))
        ]

    def slab_sem(place):
        return flow.at[WO_SEM + 1 + lax.rem(place + 2, places)]

    def slab_copies(k):
        place = lax.rem(k, places)
        copies = []
        for m, src in enumerate((wg_hbm, wu_hbm)):
            for j, w in enumerate((WIDE, ff - WIDE)):
                p = 2 * m + j
                copies.append(
                    pltpu.make_async_copy(
                        src.at[pl.ds(many(k * SLAB, SLAB), SLAB), pl.ds(j * WIDE, w)],
                        pool.at[pl.ds(many(place * (4 * SLAB), SLAB) + p * SLAB, SLAB), pl.ds(0, w)],
                        slab_sem(place),
                    )
                )
        return copies

    def start(copies):
        for c in copies:
            c.start(priority=1)

    def wait(copy, name):
        with jax.named_scope(name):
            copy.wait()

    def pool_wait(words, sem, name):
        n = words // WIDE
        if n * WIDE == words:
            region = pool.at[pl.ds(0, n), pl.ds(0, WIDE)]
        else:
            region = pool.at[pl.ds(0, words // CHUNK), pl.ds(0, CHUNK)]
        wait(pltpu.make_async_copy(region, region, sem), name)

    per_wide = WIDE // CHUNK

    def chunk_place(c):
        group = c // per_wide
        first = 6 * (1 - (group + 1) // 2) + 3 * (group // 2)
        return many(first * UNIT, UNIT), many(lax.rem(c, per_wide) * CHUNK, CHUNK)

    def chunk_copy(c):
        row, lane = chunk_place(c)
        return pltpu.make_async_copy(
            wd_hbm.at[:, pl.ds(many(c * CHUNK, CHUNK), CHUNK)], pool.at[pl.ds(row, ff), pl.ds(lane, CHUNK)], flow.at[c]
        )

    x_copy.start()
    ga_copy.start()
    turn_copy.start()
    for i in range(d // UNIT):
        wq_copy(i).start(priority=1)
    for i in range(RING):
        start(kv_copies(i))
    gm_copy.start()

    @jax.named_scope("norm")
    def norm(src, gain_ref, row0, n):
        g = gain_ref[...].astype(F32)
        gain = jnp.concatenate([g[r : r + 1] for r in range(g.shape[0])], axis=1)

        def body(i, _):
            at = pl.ds(many(row0 + i * 16, 16), 16)
            wide = src[at, :].astype(F32)
            scale = lax.rsqrt(jnp.mean(wide * wide, -1, keepdims=True) + 1e-6)
            out = (wide * scale * gain).astype(BF16)
            for k in range(slabs):
                ab[k, at, :] = out[:, k * SLAB : (k + 1) * SLAB]
            return 0

        lax.fori_loop(0, n // 16, body, 0)

    wait(x_copy, "x_wait")
    wait(ga_copy, "ga_wait")
    norm(x_s, ga_s, 0, rows)

    per = UNIT // SLAB
    for i in range(d // UNIT):
        wait(wq_copy(i), "wq_wait")
        total = None
        for j in range(per):
            term = jnp.dot(
                ab[i * per + j], pool[(WO_AT + i) * UNIT + j * SLAB : (WO_AT + i) * UNIT + (j + 1) * SLAB, :qd],
                preferred_element_type=F32,
            )
            total = term if total is None else total + term
        part[:, :qd] = total if i == 0 else part[:, :qd] + total
    wait(turn_copy, "turn_wait")
    cos, sin = turn_s[0:1, :], turn_s[1:2, :]
    blank = jnp.zeros((rows, HEAD), F32)
    for j in range(heads):
        t = part[:, j * HEAD : (j + 1) * HEAD].astype(BF16).astype(F32)
        swapped = jnp.concatenate([t[:, HEAD // 2 :], t[:, : HEAD // 2]], axis=1)
        t = (t * cos + swapped * sin).astype(BF16).astype(F32)
        side = [blank] * kv_heads
        side[j // share] = t
        t = jnp.concatenate(side + [jnp.zeros((rows, tiles * 128 - kvd), F32)], axis=1)
        for c in range(tiles):
            qs[c, pl.ds(j, rows, stride=heads), :] = t[:, c * 128 : (c + 1) * 128]

    def swap(step, half, at, got, send_sem, recv_sem):
        return pltpu.make_async_remote_copy(
            src_ref=(sent, sent2)[step].at[at], dst_ref=got[step].at[at], send_sem=send_sem, recv_sem=recv_sem,
            device_id={"tp": plan[half][step]}, device_id_type=MESH,
        )

    def arrived(words, sem):
        region = sent.at[:, pl.ds(0, words // rows)]
        pltpu.make_async_copy(region, region, sem).wait()

    half_block = BLOCK // 2
    exposed = len(GROUPS) - 1

    def rows_of(g):
        b0, b1 = GROUPS[g]
        return b0 * BATCH, (b1 - b0) * BATCH

    def first_recv(g, step, c):
        return a1_recv1.at[step, c] if g == exposed else a1_recv0.at[step, g]

    def first_send(g, step, c):
        row0, n = rows_of(g)
        for half in range(2):
            at = (pl.ds(row0, n), pl.ds(many(c * BLOCK + half * half_block, half_block), half_block))
            swap(step, half, at, (got1, got2), a1_send.at[step], first_recv(g, step, c)).start()

    def first_step(g, step, c):
        row0, n = rows_of(g)
        at = (pl.ds(row0, n), pl.ds(many(c * BLOCK, BLOCK), BLOCK))
        if g == exposed:
            with jax.named_scope("first_wait"):
                arrived(n * BLOCK, first_recv(g, step, c))
        if step == 0:
            sent2[at] = (sent[at].astype(F32) + got1[at].astype(F32)).astype(BF16)
            first_send(g, 1, c)
        else:
            x_s[at] = (x_s[at].astype(F32) + (sent2[at].astype(F32) + got2[at].astype(F32))).astype(BF16)

    def all_blocks(g, step):
        row0, n = rows_of(g)
        with jax.named_scope("all_wait"):
            arrived(n * d, first_recv(g, step, 0))
        lax.fori_loop(0, d // BLOCK, lambda c, _: first_step(g, step, c) or 0, 0)

    @jax.named_scope("gather_seen")
    def gather_seen(g):
        row0, n = rows_of(g)
        for j in range(heads):
            o = jnp.concatenate([qs[c, pl.ds(row0 * heads + j, n, stride=heads), :] for c in range(tiles)], axis=1)
            h = j // share
            seen[row0 : row0 + n, j * HEAD : (j + 1) * HEAD] = o[:, h * HEAD : (h + 1) * HEAD].astype(BF16)

    @jax.named_scope("project")
    def project(g, c):
        row0, n = rows_of(g)
        row, lane = (WO_AT + c // 2) * UNIT, lax.rem(c, 2) * BLOCK
        w = pool[pl.ds(many(row, UNIT), qd), pl.ds(many(lane, BLOCK), BLOCK)]
        at = (slice(row0, row0 + n), pl.ds(many(c * BLOCK, BLOCK), BLOCK))
        sent[at] = jnp.dot(seen[row0 : row0 + n, :], w, preferred_element_type=F32).astype(BF16)
        first_send(g, 0, c)

    def attend(i, early):
        slot = lax.rem(i + 2, RING)

        def kv_wait(j, name):
            pool_wait(BATCH * kvd * WIDE, kv_sem.at[slot, j], name)

        kv_wait(0, "k_wait")
        if not early:
            kv_wait(1, "v_wait")
        at = kv_at(i)
        ws = []
        for j in range(BATCH):
            mine = pl.ds(many((i * BATCH + j) * heads, 8), heads)
            q = jnp.concatenate([qs[c, mine, :] for c in range(tiles)], axis=1)[:, :kvd].astype(BF16)
            scores = jnp.dot(q, pool[pl.ds(at + j * kvd, kvd), :WIDE], preferred_element_type=F32) * HEAD**-0.5
            top = jnp.max(scores, -1, keepdims=True)
            e = jnp.exp(scores - top)
            ws.append(e * (1 / jnp.sum(e, -1, keepdims=True)))
        w = jnp.concatenate(ws, 0).astype(BF16)
        if early:
            kv_wait(1, "v_wait")
        o = lax.dot_general(w, pool[pl.ds(at + UNIT, BATCH * kvd), :WIDE], (((1,), (1,)), ((), ())), preferred_element_type=F32)
        for j in range(BATCH):
            t = o[j * heads : (j + 1) * heads, j * kvd : (j + 1) * kvd]
            t = jnp.concatenate([t, jnp.zeros((heads, tiles * 128 - kvd), F32)], axis=1)
            for c in range(tiles):
                qs[c, pl.ds(many((i * BATCH + j) * heads, 8), heads), :] = t[:, c * 128 : (c + 1) * 128]

        @pl.when(i + RING < batches)
        def _():
            start(kv_copies(i + RING))

        @pl.when(i == 8)
        def _():
            start(wo_copies())

        @pl.when(i >= batches - RING)
        def _():
            start(slab_copies(i - (batches - RING)))

        end0 = GROUPS[0][1]

        @pl.when(i == end0 - 1)
        def _():
            pool_wait(qd * d, flow.at[WO_SEM], "wo_wait")
            pl.semaphore_wait(barrier, 2)
            gather_seen(0)
            lax.fori_loop(0, d // BLOCK, lambda c, _: project(0, c) or 0, 0)

        @pl.when(i == end0 + 1)
        def _():
            all_blocks(0, 0)

        return 0

    lax.fori_loop(0, GROUPS[0][1], lambda i, _: attend(i, True), 0)
    lax.fori_loop(GROUPS[0][1], batches - 1, lambda i, _: attend(i, False), 0)
    lax.fori_loop(batches - 1, batches, lambda i, _: attend(i, True), 0)

    gather_seen(exposed)
    blocks = d // BLOCK

    def project_body(c, _):
        project(exposed, c)

        @pl.when(c == blocks - 1)
        def _():
            for k in range(RING, places):
                start(slab_copies(k))

        return 0

    lax.fori_loop(0, blocks, project_body, 0)
    all_blocks(exposed - 1, 1)
    gm_copy.wait()
    norm(x_s, gm_s, *rows_of(exposed - 1))
    accu[...] = jnp.zeros_like(accu)
    part[:, :ff] = jnp.zeros((rows, ff), F32)

    @jax.named_scope("slab")
    def slab_dots(k, row0, n):
        place = lax.rem(k, places)
        mine = slice(row0, row0 + n)
        lhs = ab[k, mine, :]
        for m, acc in enumerate((part, accu)):
            for j, w in enumerate((WIDE, ff - WIDE)):
                at = pl.ds(many(place * (4 * SLAB), SLAB) + (2 * m + j) * SLAB, SLAB)
                acc[mine, j * WIDE : j * WIDE + w] += jnp.dot(lhs, pool[at, :w], preferred_element_type=F32)

    def slab_wait(k):
        pool_wait(2 * SLAB * ff, slab_sem(lax.rem(k, places)), "slab_wait")

    def refill(k):
        @pl.when(k < slabs - places)
        def _():
            start(slab_copies(k + places))

        for after, first, last in ((4, 0, per_wide), (6, per_wide, 2 * per_wide), (7, 2 * per_wide, chunks)):

            @pl.when(k == after)
            def _():
                for c in range(first, last):
                    start([chunk_copy(c)])

    last_row, last_rows = rows_of(exposed)

    def early_body(k, _):
        slab_wait(k)
        slab_dots(k, 0, last_row)

        @pl.when(k == 0)
        def _():
            lax.fori_loop(0, blocks, lambda c, _: first_step(exposed, 0, c) or 0, 0)

        return 0

    lax.fori_loop(0, EARLY, early_body, 0)
    lax.fori_loop(0, blocks, lambda c, _: first_step(exposed, 1, c) or 0, 0)
    norm(x_s, gm_s, last_row, last_rows)
    for step in range(2):
        arrived(rows * d, a1_send.at[step])

    def late_body(k, _):
        slab_dots(k, last_row, last_rows)
        refill(k)
        return 0

    lax.fori_loop(0, EARLY, late_body, 0)

    def slab_body(k, _):
        slab_wait(k)
        slab_dots(k, 0, rows)
        refill(k)
        return 0

    lax.fori_loop(EARLY, slabs, slab_body, 0)

    def hidden_body(c, _):
        at = pl.ds(many(c * 384, 128), 384)
        got1[:, at] = (jax.nn.silu(part[:, at]) * accu[:, at]).astype(BF16)
        return 0

    lax.fori_loop(0, ff // 384, hidden_body, 0)

    side = CHUNK // 2

    def columns_of(c, half):
        return pl.ds(many(c * CHUNK + half * side, side), side)

    def full_send(c, step):
        for half in range(2):
            at = (slice(None), columns_of(c, half))
            swap(step, half, at, (got1b, y_s), a2_send.at[step], a2_recv.at[c, step]).start()

    @jax.named_scope("full_step")
    def full_step(c, step):
        arrived(rows * CHUNK, a2_recv.at[c, step])
        at = (slice(None), pl.ds(many(c * CHUNK, CHUNK), CHUNK))
        if step == 0:
            sent2[at] = (sent[at].astype(F32) + got1b[at].astype(F32)).astype(BF16)
            full_send(c, 1)
        else:
            y_s[at] = (x_s[at].astype(F32) + (sent2[at].astype(F32) + y_s[at].astype(F32))).astype(BF16)

    row2 = rows // 2

    def halved_send(c, step):
        for half in range(2):
            row = (1 - kept[half]) * row2 if step == 0 else kept[half] * row2
            at = (pl.ds(many(row, 32), row2), columns_of(c, half))
            pltpu.make_async_remote_copy(
                src_ref=(sent, sent2, y_s)[step].at[at], dst_ref=(got1b, y_s, y_s)[step].at[at], send_sem=a2_send.at[step],
                recv_sem=a2_back.at[c] if step == 2 else a2_recv.at[c, step],
                device_id={"tp": plan[half][step % 2]}, device_id_type=MESH,
            ).start()

    @jax.named_scope("halved_step")
    def halved_step(c, step):
        arrived(row2 * CHUNK, a2_back.at[c] if step == 2 else a2_recv.at[c, step])
        if step == 2:
            return
        for half in range(2):
            at = (pl.ds(many(kept[half] * row2, 32), row2), columns_of(c, half))
            if step == 0:
                sent2[at] = (part[at] + got1b[at].astype(F32)).astype(BF16)
            else:
                y_s[at] = (x_s[at].astype(F32) + (sent2[at].astype(F32) + y_s[at].astype(F32))).astype(BF16)
        halved_send(c, step + 1)

    def down(i):
        wait(chunk_copy(i), "chunk_wait")
        row, lane = chunk_place(i)
        return jnp.dot(got1[:, :ff], pool[pl.ds(row, ff), pl.ds(lane, CHUNK)], preferred_element_type=F32)

    def down_body(i, _):
        for step in (2, 1, 0):
            at = (step + 1) * LAG

            @pl.when((i >= at) & (i < HALVED + at))
            def _():
                halved_step(i - at, step)

            if step < 2:

                @pl.when((i >= HALVED + at) & (i < chunks + at))
                def _():
                    full_step(i - at, step)

        @pl.when(i < HALVED)
        def _():
            part[:, pl.ds(many(i * CHUNK, CHUNK), CHUNK)] = down(i)
            for half in range(2):
                at = (pl.ds(many((1 - kept[half]) * row2, 32), row2), columns_of(i, half))
                sent[at] = part[at].astype(BF16)
            halved_send(i, 0)

        @pl.when((i >= HALVED) & (i < chunks))
        def _():
            sent[:, pl.ds(many(i * CHUNK, CHUNK), CHUNK)] = down(i).astype(BF16)
            full_send(i, 0)

        return 0

    lax.fori_loop(0, max(chunks + 2 * LAG, HALVED + 3 * LAG), down_body, 0)
    whole = chunks - HALVED
    for step, n in enumerate((HALVED * row2 + whole * rows, HALVED * row2 + whole * rows, HALVED * row2)):
        arrived(n * CHUNK, a2_send.at[step])


def solution(mesh):
    def step(x, k_cache, v_cache, gain_a, wq, wo, gain_m, w_gate, w_up, w_down):
        rows, d = x.shape
        _, cache, kv_heads, head = k_cache.shape
        heads, ff = wq.shape[1] // head, w_gate.shape[1]
        keys, values = (t.transpose(0, 2, 3, 1).reshape(rows * kv_heads * head, cache) for t in (k_cache, v_cache))
        half = head // 2
        angle = np.float32(cache - 1) * np.float32(THETA) ** (-np.arange(half, dtype=np.float32) / np.float32(half))
        cos, sin = np.cos(angle.astype(np.float32)), np.sin(angle.astype(np.float32))
        turn = np.zeros((8, head), np.float32)
        turn[0], turn[1] = np.concatenate([cos, cos]), np.concatenate([-sin, sin])
        chunks = d // CHUNK
        dims = (rows, d, cache, heads, kv_heads, ff)
        dma = pltpu.SemaphoreType.DMA
        return pl.pallas_call(
            functools.partial(kernel, dims),
            out_shape=pltpu.VMEM((rows, d), BF16),
            in_specs=[pl.BlockSpec(memory_space=pltpu.HBM)] * 11,
            out_specs=pl.BlockSpec(memory_space=pltpu.VMEM),
            scratch_shapes=[
                pltpu.VMEM((UNITS * UNIT, PITCH), BF16),
                pltpu.VMEM((rows, d), BF16),
                pltpu.VMEM((d // 128, 128), BF16),
                pltpu.VMEM((d // 128, 128), BF16),
                pltpu.VMEM((8, head), F32),
                pltpu.VMEM((d // SLAB, rows, SLAB), BF16),
                pltpu.VMEM((-(-kv_heads * head // 128), rows * heads, 128), F32),
                pltpu.VMEM((rows, heads * head), BF16),
                pltpu.VMEM((rows, d), F32),
                pltpu.VMEM((rows, ff), F32),
                pltpu.VMEM((rows, d), BF16),
                pltpu.VMEM((rows, d), BF16),
                pltpu.VMEM((rows, d), BF16),
                pltpu.VMEM((rows, d), BF16),
                pltpu.VMEM((rows, d), BF16),
                dma((4,)),
                dma((chunks,)),
                dma((RING, 2)),
                dma((2,)),
                dma((2, len(GROUPS) - 1)),
                dma((2, d // BLOCK)),
                dma((3,)),
                dma((chunks, 2)),
                dma((HALVED,)),
            ],
            compiler_params=pltpu.CompilerParams(
                collective_id=0, has_side_effects=True, vmem_limit_bytes=66350000
            ),
        )(x, keys, values, gain_a.reshape(d // 128, 128), wq, wo, gain_m.reshape(d // 128, 128), w_gate, w_up, w_down, turn)

    states, cache, columns, rows_of = P("dp", None), P("dp", None, "tp", None), P(None, "tp"), P("tp", None)
    return jax.shard_map(
        step,
        mesh=mesh,
        in_specs=(states, cache, cache, P(None), columns, rows_of, P(None), columns, columns, rows_of),
        out_specs=states,
        check_vma=False,
    )
```
